512 devices in a mesh: row: 16 (over z_hi, y), col: 4 (over x), cuts: 8 (over z_lo, core).
Axes of the slice: x: 4, y: 4, z: 16 (z_hi: 4, z_lo: 4; z = z_hi * 4 + z_lo), core: 2. Of those that a mesh axis runs over, the one named last changes fastest.
Arguments:
- warm: float32 [40, 131072], P('cuts', ('row', 'col')), may hold values from -6 to 6
- tiles: float32 [22016, 128, 128], P(('row', 'col', 'cuts')), may hold values from -0.125 to 0.125
- tile_rows: int32 [22016], P(('row', 'col', 'cuts')), may hold values from -1 to 1023, as said below
- tile_cols: int32 [22016], P(('row', 'col', 'cuts')), may hold values from 0 to 1023, as said below
Outputs:
- basis: float32 [40, 131072], P('cuts', ('row', 'col'))
- residual: float32 [40, 131072], P('cuts', ('row', 'col'))
The draws below stay inside these ranges and needn't reach their ends.
Inputs may be any that keep to these rules, and one draw needn't show every extreme that they name: `tile_rows`: slots come in groups of 344; group r * (size of col) + c belongs to the grid position with row index r and column index c. A group's tiles lie in the block rows r * (size of col) * 16 up to (r + 1) * (size of col) * 16 - 1, and in block columns j with (j // 16) % (size of col) = c. No block appears twice. In each group the live slots come first and fill at least half of it; some group is full. Block rows hold uneven numbers of tiles. `tile_cols`: see tile_rows; an empty slot's column is that of some block the group may hold.
All inputs are finite; a program needn't handle non-finite values.
Results may differ from the reference program's by a relative error of at most 0.0003.
Values sent between devices are 32-bit elements; how exact they have to be, the bound alone decides.
A program may use at most 64 MiB of HBM per device.

```python
import jax
import jax.numpy as jnp
from jax import lax

K = 40
BLOCK = 128
TILES_ROW = 16
SEG_BLOCKS = 16
SLOTS = 344
BLOCK_ROWS = 1024
ITEMS = 131072
SLOTS_ALL = 22016
N_ROW = 16
N_COL = 4


def tile_pattern(key):
    devices = N_ROW * N_COL
    key = jax.random.fold_in(key, 4211)
    score_key, count_key, full_key = jax.random.split(key, 3)
    local_rows = N_COL * SEG_BLOCKS
    local_cols = N_ROW * SEG_BLOCKS
    candidates = local_rows * local_cols
    upper = max(2, (1 << 30) // candidates)
    scores = jax.random.randint(score_key, (devices, candidates), 0, upper) * candidates + jnp.arange(candidates, dtype=jnp.int32)[None, :]
    order = jnp.argsort(scores, axis=1, stable=True)[:, :SLOTS].astype(jnp.int32)
    counts = jax.random.randint(count_key, (devices,), SLOTS // 2, SLOTS + 1)
    busiest = jax.random.randint(full_key, (), 0, devices)
    counts = jnp.where(jnp.arange(devices) == busiest, SLOTS, counts)
    device = jnp.arange(devices, dtype=jnp.int32)[:, None]
    row_index = device // N_COL
    col_index = device % N_COL
    lrow = order // local_cols
    lcol = order % local_cols
    grow = row_index * N_COL * SEG_BLOCKS + lrow
    gcol = (lcol // SEG_BLOCKS * N_COL + col_index) * SEG_BLOCKS + lcol % SEG_BLOCKS
    live = jnp.arange(SLOTS, dtype=jnp.int32)[None, :] < counts[:, None]
    rows = jnp.where(live, grow, -1)
    return (rows.reshape(-1).astype(jnp.int32), gcol.reshape(-1).astype(jnp.int32))


def draw_tile_rows(key, part):
    return tile_pattern(key)[0]


def draw_tile_cols(key, part):
    return tile_pattern(key)[1]


def levels(own_key, extent, shards, smallest, high):
    def one(axis_at, blocks):
        steps = jax.random.uniform(jax.random.fold_in(jax.random.fold_in(own_key, 6), axis_at), (blocks,), jnp.float32, smallest / len(shards), high / len(shards))
        return jnp.repeat(jnp.exp(steps), extent[axis_at] // blocks).reshape((-1,) + (1,) * (len(extent) - axis_at - 1))

    gain = one(*shards[0])
    for cut in shards[1:]:
        gain = gain * one(*cut)
    return gain


def scatter_about(stream_key, shape, deviation, limit, cuts=(), held_as=jnp.bfloat16):
    gain = levels(stream_key, shape, cuts, -0.22, 0.18) if cuts else 1.0
    entries = jax.random.normal(stream_key, shape, jnp.float32) * deviation * gain
    return jnp.minimum(jnp.maximum(entries, -limit), limit).astype(held_as)


def setup_inputs(seed: int = 0) -> dict:
    keys = jax.random.split(jax.random.key(seed), 5)
    warm = scatter_about(keys[0], (K, ITEMS), 1.0, 6.0, ((0, 8), (1, 64)), jnp.float32)
    tiles = scatter_about(keys[1], (SLOTS_ALL, BLOCK, BLOCK), (TILES_ROW * BLOCK) ** -0.5, 0.125, ((0, 512),), jnp.float32)
    tile_rows = draw_tile_rows(jax.random.fold_in(keys[4], 71), 0)
    tile_cols = draw_tile_cols(jax.random.fold_in(keys[4], 71), 0)
    return {"warm": warm, "tiles": tiles, "tile_rows": tile_rows, "tile_cols": tile_cols}


def multiply(vectors, tiles, tile_rows, tile_cols):
    count_rows = vectors.shape[0]
    blocks = vectors.reshape(count_rows, BLOCK_ROWS, BLOCK)
    groups = N_ROW * N_COL

    def accumulate(total, pieces):
        tile_group, row_group, col_group = pieces
        picked = jnp.take(blocks, col_group.astype(jnp.int32), axis=1)
        prods = jnp.einsum('suv,ksv->ksu', tile_group, picked, precision=lax.Precision.HIGHEST)
        live = (row_group >= 0).astype(total.dtype)
        prods = prods * live[None, :, None]
        target = jnp.maximum(row_group, 0).astype(jnp.int32)
        summed = jax.ops.segment_sum(jnp.transpose(prods, (1, 0, 2)), target, num_segments=BLOCK_ROWS)
        return (total + summed, None)
    start = jnp.zeros((BLOCK_ROWS, count_rows, BLOCK), vectors.dtype)
    total, _ = lax.scan(accumulate, start, (tiles.reshape(groups, SLOTS, BLOCK, BLOCK), tile_rows.reshape(groups, SLOTS), tile_cols.reshape(groups, SLOTS)))
    return jnp.transpose(total, (1, 0, 2)).reshape(count_rows, ITEMS)

def reference(warm, tiles, tile_rows, tile_cols):
    image = multiply(warm, tiles, tile_rows, tile_cols)
    gram = jnp.dot(image.astype(jnp.float32), image.T.astype(jnp.float32), precision=lax.Precision.HIGHEST, preferred_element_type=jnp.float32) / ITEMS
    lower = jnp.linalg.cholesky(gram)
    basis = lax.linalg.triangular_solve(lower, image, left_side=True, lower=True)
    product = multiply(basis, tiles, tile_rows, tile_cols)
    projected = jnp.dot(basis.astype(jnp.float32), product.T.astype(jnp.float32), precision=lax.Precision.HIGHEST, preferred_element_type=jnp.float32) / ITEMS
    residual = product - jnp.dot(projected.T.astype(jnp.float32), basis.astype(jnp.float32), precision=lax.Precision.HIGHEST, preferred_element_type=jnp.float32)
    return (basis, residual)
```

```python
import jax
import jax.numpy as jnp
from jax import lax
from jax.experimental import pallas as pl
from jax.experimental.pallas import tpu as pltpu
from jax.sharding import PartitionSpec as P

MESH = pl.DeviceIdType.MESH
NZ = 16
NY = 4
NX = 4
NZL = 4
ROWS = 80
SLOTS = 43
PAD = 48
KALL = 40
OUT = 64
F32 = jnp.float32
BF16 = jnp.bfloat16


def split(v):
    hi = v.astype(BF16)
    lo = (v - hi.astype(F32)).astype(BF16)
    return hi, lo


def dot_nt(a, b):
    return lax.dot_general(a, b, (((1,), (1,)), ((), ())), preferred_element_type=F32)


def rem(a, n):
    return lax.rem(a, jnp.int32(n))


def div(a, n):
    return lax.div(a, jnp.int32(n))


def apply_kernel(
    x_ref, tiles_hbm, start_ref, local_ref, out_ref, whole_ref,
    tiles_v, panel, prods, y_ref, part, far, near, tail, gathered,
    tile_sem, send_sem, zr, zl_sem, yf, yh, d2d, core_s, core_r, x_s, x_r, q_s, q_r,
):
    row = lax.axis_index("row")
    x = lax.axis_index("col")
    cut = lax.axis_index("cuts")
    zh, y = div(row, NY), rem(row, NY)
    zlo, c = div(cut, 2), rem(cut, 2)
    z = zh * NZL + zlo

    def dev(zz, yy, xx, cc):
        return {"row": div(zz, NZL) * NY + yy, "col": xx, "cuts": rem(zz, NZL) * 2 + cc}

    right_z, left_z = rem(z + 1, NZ), rem(z + NZ - 1, NZ)
    up, down = rem(y + 1, NY), rem(y + NY - 1, NY)
    far_y = rem(y + 2, NY)
    xr, xl, xf = rem(x + 1, NX), rem(x + NX - 1, NX), rem(x + 2, NX)
    d_zr, d_zl = dev(right_z, y, x, c), dev(left_z, y, x, c)
    d_up, d_down = dev(z, up, x, c), dev(z, down, x, c)
    d_xr, d_xl = dev(z, y, xr, c), dev(z, y, xl, c)
    d_core = dev(z, y, x, 1 - c)
    d_q = [dev(zh * NZL + rem(zlo + d, NZL), y, x, c) for d in (1, 2, 3)]
    peers = [d_zr, d_zl, d_up, d_down, d_xr, d_xl, d_core] + d_q

    tile_copy = pltpu.make_async_copy(tiles_hbm, tiles_v, tile_sem)
    tile_copy.start()

    barrier = pltpu.get_barrier_semaphore()
    for p in peers:
        pl.semaphore_signal(barrier, inc=1, device_id=p, device_id_type=MESH)
    pl.semaphore_wait(barrier, len(peers))

    def block(zz, yy, cc, part_at=0, size=ROWS):
        index = (div(zz, NZL) * NY + yy) * 8 + rem(zz, NZL) * 2 + cc
        return panel.at[pl.ds(pl.multiple_of(index * ROWS + part_at, 8), size)]

    def copy(src, dst, s, r, d):
        return pltpu.make_async_remote_copy(
            src_ref=src, dst_ref=dst, send_sem=s, recv_sem=r, device_id=d, device_id_type=MESH
        )

    def zsrc(o):
        return rem(z + NZ - o, NZ)

    def emit(o):
        b = block(zsrc(o), y, c)
        src = x_ref if o == 0 else b
        copy(src, b, send_sem, yf.at[o], d_up).start()
        copy(src, b, send_sem, yf.at[NZ + o], d_down).start()
        copy(src, b, send_sem, d2d, d_core).start()

    def y_arrive(o):
        b = block(zsrc(o), down, c)
        copy(b, b, send_sem, yf.at[o], d_up).wait_recv()
        h = block(zsrc(o), down, c, 0, ROWS // 2)
        copy(h, h, send_sem, yh.at[o], d_up).start()
        copy(b, b, send_sem, d2d, d_core).start()
        b = block(zsrc(o), up, c)
        copy(b, b, send_sem, yf.at[NZ + o], d_down).wait_recv()
        h = block(zsrc(o), up, c, ROWS // 2, ROWS // 2)
        copy(h, h, send_sem, yh.at[NZ + o], d_down).start()
        copy(b, b, send_sem, d2d, d_core).start()

    def h_arrive(o):
        h = block(zsrc(o), far_y, c, 0, ROWS // 2)
        copy(h, h, send_sem, yh.at[o], d_up).wait_recv()
        h = block(zsrc(o), far_y, c, ROWS // 2, ROWS // 2)
        copy(h, h, send_sem, yh.at[NZ + o], d_down).wait_recv()
        b = block(zsrc(o), far_y, c)
        copy(b, b, send_sem, d2d, d_core).start()

    own = block(z, y, c)
    copy(x_ref, own, send_sem, zr.at[0], d_zr).start()
    copy(x_ref, own, send_sem, zl_sem.at[0], d_zl).start()
    emit(0)
    own[...] = x_ref[...]
    prods[...] = jnp.zeros_like(prods)
    before, older = [0], []
    for t in range(8):
        now = [t + 1]
        b = block(zsrc(t + 1), y, c)
        copy(b, b, send_sem, zr.at[t], d_zr).wait_recv()
        if t < 7:
            copy(b, b, send_sem, zr.at[t + 1], d_zr).start()
            b = block(zsrc(15 - t), y, c)
            copy(b, b, send_sem, zl_sem.at[t], d_zl).wait_recv()
            if t < 6:
                copy(b, b, send_sem, zl_sem.at[t + 1], d_zl).start()
            now.append(15 - t)
        for o in now:
            emit(o)
        for o in before:
            y_arrive(o)
        for o in older:
            h_arrive(o)
        before, older = now, before
    for o in before:
        y_arrive(o)
    for o in older + before:
        h_arrive(o)
    half = panel.at[pl.ds(0, 64 * ROWS)]
    copy(half, half, send_sem, d2d, d_core).wait_recv()
    most = panel.at[pl.ds(0, 127 * ROWS)]
    copy(most, most, send_sem, d2d, d_core).wait_send()

    tile_copy.wait()

    def slot(s):
        p_hi, p_lo = split(panel[pl.ds(start_ref[s], KALL, stride=16), :])
        t_hi, t_lo = split(tiles_v[s])
        prods[pl.ds(s, KALL, stride=PAD), :] = (
            dot_nt(p_hi, t_hi) + (dot_nt(p_lo, t_hi) + dot_nt(p_hi, t_lo))
        )

    def slots(i, carry):
        for j in range(7):
            slot(i * 7 + j)
        return carry

    lax.fori_loop(0, 6, slots, 0)
    slot(42)

    onehot = (
        lax.broadcasted_iota(jnp.int32, (OUT, 2 * PAD), 0) == local_ref[...]
    ).astype(F32).astype(BF16)

    half_rows = 20
    core_copies = []
    for q in range(NZL):
        for par in range(2):
            for kk in range(5):
                k = q * 10 + par * 5 + kk
                hi, lo = split(prods[pl.ds(k * PAD, PAD), :])
                y_ref[par, q * 5 + kk] = jnp.dot(
                    onehot, jnp.concatenate([hi, lo], axis=0), preferred_element_type=F32
                )
        cp = copy(
            y_ref.at[1 - c, pl.ds(q * 5, 5)], part.at[pl.ds(q * 5, 5)],
            core_s.at[q], core_r.at[q], d_core,
        )
        cp.start()
        core_copies.append(cp)

    total = y_ref.at[c]
    for q in range(NZL):
        core_copies[q].wait_recv()
        rows_q = pl.ds(q * 5, 5)
        total[rows_q] = total[rows_q] + part[rows_q]

    def seg(xx, first):
        return total.at[pl.ds(first, 10), pl.ds(pl.multiple_of(xx * 16, 16), 16)]

    far_r = copy(seg(xf, 0), far.at[0], x_s.at[0], x_r.at[0], d_xr)
    far_l = copy(seg(xf, 10), far.at[1], x_s.at[1], x_r.at[1], d_xl)
    near_rb = copy(seg(xr, 10), near.at[0, pl.ds(10, 10)], x_s.at[2], x_r.at[2], d_xr)
    near_la = copy(seg(xl, 0), near.at[1, pl.ds(0, 10)], x_s.at[3], x_r.at[3], d_xl)
    near_ra = copy(seg(xr, 0), near.at[0, pl.ds(0, 10)], x_s.at[4], x_r.at[4], d_xr)
    near_lb = copy(seg(xl, 10), near.at[1, pl.ds(10, 10)], x_s.at[5], x_r.at[5], d_xl)
    far_r.start()
    far_l.start()
    near_rb.start()
    near_la.start()
    far_r.wait_recv()
    seg(xr, 0)[...] = seg(xr, 0)[...] + far[0]
    near_ra.start()
    far_l.wait_recv()
    seg(xl, 10)[...] = seg(xl, 10)[...] + far[1]
    near_lb.start()
    near_la.wait_recv()
    near_ra.wait_recv()
    tail[pl.ds(0, 10)] = seg(x, 0)[...] + near[0, pl.ds(0, 10)] + near[1, pl.ds(0, 10)]
    near_rb.wait_recv()
    near_lb.wait_recv()
    tail[pl.ds(10, 10)] = seg(x, 10)[...] + near[0, pl.ds(10, 10)] + near[1, pl.ds(10, 10)]

    q_copies = []
    for d in (1, 2, 3):
        to = rem(zlo + d, NZL)
        cp = copy(
            tail.at[pl.ds(to * 5, 5)], gathered.at[d - 1], q_s.at[d - 1], q_r.at[d - 1], d_q[d - 1]
        )
        cp.start()
        q_copies.append(cp)
    whole_ref[...] = panel[pl.ds(pl.multiple_of(row * 8 * ROWS, 8), 8 * ROWS), :]
    acc = tail[pl.ds(zlo * 5, 5)]
    for cp in q_copies:
        cp.wait_recv()
    out_ref[...] = acc + gathered[0] + gathered[1] + gathered[2]

    for cp in core_copies + [far_r, far_l, near_rb, near_la, near_ra, near_lb] + q_copies:
        cp.wait_send()


def apply_call(vectors, tiles, start, local):
    dma = pltpu.SemaphoreType.DMA
    vmem = pl.BlockSpec(memory_space=pltpu.VMEM)
    return pl.pallas_call(
        apply_kernel,
        name="operator_apply",
        out_shape=(
            jax.ShapeDtypeStruct((5, 16, 128), F32),
            jax.ShapeDtypeStruct((8 * ROWS, 128), F32),
        ),
        in_specs=[
            vmem,
            pl.BlockSpec(memory_space=pl.ANY),
            pl.BlockSpec(memory_space=pltpu.SMEM),
            vmem,
        ],
        out_specs=(vmem, vmem),
        scratch_shapes=[
            pltpu.VMEM((SLOTS, 128, 128), F32),
            pltpu.VMEM((128 * ROWS, 128), F32),
            pltpu.VMEM((KALL * PAD, 128), F32),
            pltpu.VMEM((2, 20, OUT, 128), F32),
            pltpu.VMEM((20, OUT, 128), F32),
            pltpu.VMEM((2, 10, 16, 128), F32),
            pltpu.VMEM((2, 20, 16, 128), F32),
            pltpu.VMEM((20, 16, 128), F32),
            pltpu.VMEM((3, 5, 16, 128), F32),
            dma, dma, dma((8,)), dma((7,)), dma((32,)), dma((32,)), dma,
            dma((4,)), dma((4,)), dma((6,)), dma((6,)), dma((3,)), dma((3,)),
        ],
        compiler_params=pltpu.CompilerParams(collective_id=0, has_side_effects=True),
    )(vectors, tiles, start, local)


def hdot(a, b):
    return jnp.dot(a, b, precision=lax.Precision.HIGHEST, preferred_element_type=F32)


def shards(warm, tiles, tile_rows, tile_cols):
    items = 131072
    local = tile_rows - lax.axis_index("row") * OUT
    local = jnp.pad(local, (0, PAD - SLOTS), constant_values=-1)
    local = jnp.concatenate([local, local]).reshape(1, 2 * PAD)
    start = tile_cols // 64 * (8 * ROWS) + tile_cols % 16
    image, _ = apply_call(warm.reshape(ROWS, 128), tiles, start, local)
    product, whole = apply_call(image.reshape(ROWS, 128), tiles, start, local)
    whole = whole.reshape(KALL, 2048)
    product = lax.all_gather(product.reshape(5, 2048), "cuts", axis=0, tiled=True)
    sums = jnp.concatenate([hdot(whole, whole.T), hdot(whole, product.T)], axis=1)
    sums = lax.psum(sums, ("row", "col")) / items
    gram, mixed = sums[:, :KALL], sums[:, KALL:]
    lower = jnp.linalg.cholesky(gram)
    inverse = lax.linalg.triangular_solve(
        lower, jnp.eye(KALL, dtype=F32), left_side=True, lower=True
    )
    projected = hdot(inverse, hdot(mixed, inverse.T))
    mine = lax.dynamic_slice_in_dim(inverse, lax.axis_index("cuts") * 5, 5, 0)
    basis = hdot(mine, whole)
    columns = lax.dynamic_slice_in_dim(projected, lax.axis_index("cuts") * 5, 5, 1)
    residual = hdot(mine, product) - hdot(hdot(columns.T, inverse), whole)
    return (basis, residual)


def solution(mesh):
    return jax.shard_map(
        shards,
        mesh=mesh,
        in_specs=(
            P("cuts", ("row", "col")),
            P(("row", "col", "cuts"), None, None),
            P(("row", "col", "cuts")),
            P(("row", "col", "cuts")),
        ),
        out_specs=(P("cuts", ("row", "col")), P("cuts", ("row", "col"))),
        check_vma=False,
    )
```

```python
import jax
import jax.numpy as jnp
from jax import lax
from jax.experimental import pallas as pl
from jax.experimental.pallas import tpu as pltpu
from jax.sharding import PartitionSpec as P

MESH = pl.DeviceIdType.MESH
NZ = 16
NY = 4
NX = 4
NZL = 4
ROWS = 80
SLOTS = 43
PAD = 48
KALL = 40
KLOC = 5
OUT = 64
ITEMS = 131072
F32 = jnp.float32
BF16 = jnp.bfloat16


def split(v):
    hi = v.astype(BF16)
    lo = (v - hi.astype(F32)).astype(BF16)
    return hi, lo


def dot_nt(a, b):
    return lax.dot_general(a, b, (((1,), (1,)), ((), ())), preferred_element_type=F32)


def exact_nt(a, b):
    return lax.dot_general(
        a, b, (((1,), (1,)), ((), ())),
        precision=lax.Precision.HIGHEST, preferred_element_type=F32,
    )


def exact(a, b):
    return jnp.dot(a, b, precision=lax.Precision.HIGHEST, preferred_element_type=F32)


def rem(a, n):
    return lax.rem(a, jnp.int32(n))


def div(a, n):
    return lax.div(a, jnp.int32(n))


def inverse_factor(gram):
    row = lax.broadcasted_iota(jnp.int32, (KALL, 128), 0)
    lane = lax.broadcasted_iota(jnp.int32, (KALL, 128), 1)
    m = jnp.where(lane < KALL, gram, 0.0) + (lane == row + 64).astype(F32)
    for j in range(KALL):
        d = m[j : j + 1, j : j + 1]
        r0 = lax.rsqrt(d)
        scale = r0 * (1.5 - 0.5 * d * r0 * r0)
        pivot = m[j : j + 1, :] * scale
        column = m[:, j : j + 1] * scale
        m = jnp.where(row > j, m - column * pivot, jnp.where(row == j, pivot, m))
    return m[:, 64 : 64 + KALL]


def kernel(
    x_ref, tiles_hbm, start_ref, local_ref, basis_ref, residual_ref,
    tiles_v, panel_a, panel_b, prods, y_ref, part, far, near, tail, mixed, gathered, total_u, image,
    product, basis_all, gsum, psum, tile_sem, ag_send, zr_s, zl_s, yf, yh, d2d,
    core_s, core_r, x_s, x_r, q_s, q_r, w_s, w_r, g_s, g_r, p_s, p_r,
):
    row = lax.axis_index("row")
    x = lax.axis_index("col")
    cut = lax.axis_index("cuts")
    zh, y = div(row, NY), rem(row, NY)
    zlo, c = div(cut, 2), rem(cut, 2)
    z = zh * NZL + zlo

    def dev(zz, yy, xx, cc):
        return {"row": div(zz, NZL) * NY + yy, "col": xx, "cuts": rem(zz, NZL) * 2 + cc}

    up, down, far_y = rem(y + 1, NY), rem(y + NY - 1, NY), rem(y + 2, NY)
    xr, xl, xf = rem(x + 1, NX), rem(x + NX - 1, NX), rem(x + 2, NX)
    d_zr, d_zl = dev(rem(z + 1, NZ), y, x, c), dev(rem(z + NZ - 1, NZ), y, x, c)
    d_x = [dev(z, y, rem(x + d, NX), c) for d in (1, 2, 3)]
    d_y = [dev(z, rem(y + d, NY), x, c) for d in (1, 2, 3)]
    d_up, d_down, d_xr, d_xl = d_y[0], d_y[2], d_x[0], d_x[2]
    d_core = dev(z, y, x, 1 - c)
    d_q = [dev(zh * NZL + rem(zlo + d, NZL), y, x, c) for d in (1, 2, 3)]
    d_h = [dev(rem(zh + d, 4) * NZL + zlo, y, x, c) for d in (1, 2, 3)]
    peers = [d_zr, d_zl, d_core] + d_x + d_y + d_q + d_h

    tile_copy = pltpu.make_async_copy(tiles_hbm, tiles_v, tile_sem)
    tile_copy.start()

    barrier = pltpu.get_barrier_semaphore()
    for p in peers:
        pl.semaphore_signal(barrier, inc=1, device_id=p, device_id_type=MESH)
    pl.semaphore_wait(barrier, len(peers))

    def copy(src, dst, s, r, d):
        return pltpu.make_async_remote_copy(
            src_ref=src, dst_ref=dst, send_sem=s, recv_sem=r, device_id=d, device_id_type=MESH
        )

    def zsrc(o):
        return rem(z + NZ - o, NZ)

    def gather(n, x_ref, panel, after_z):
        send_sem = ag_send.at[n]

        def block(zz, yy, part_at=0, size=ROWS):
            index = (div(zz, NZL) * NY + yy) * 8 + rem(zz, NZL) * 2 + c
            return panel.at[pl.ds(pl.multiple_of(index * ROWS + part_at, 8), size)]

        def emit(o):
            b = block(zsrc(o), y)
            src = x_ref if o == 0 else b
            copy(src, b, send_sem, yf.at[n, o], d_up).start()
            copy(src, b, send_sem, yf.at[n, NZ + o], d_down).start()
            copy(src, b, send_sem, d2d.at[n, 0], d_core).start()

        def y_arrive(o):
            for at, side, d in ((0, down, d_up), (1, up, d_down)):
                b = block(zsrc(o), side)
                copy(b, b, send_sem, yf.at[n, at * NZ + o], d).wait_recv()
                h = block(zsrc(o), side, at * (ROWS // 2), ROWS // 2)
                copy(h, h, send_sem, yh.at[n, at * NZ + o], d).start()
                copy(b, b, send_sem, d2d.at[n, 1], d_core).start()

        def h_arrive(o):
            for at, d in ((0, d_up), (1, d_down)):
                h = block(zsrc(o), far_y, at * (ROWS // 2), ROWS // 2)
                copy(h, h, send_sem, yh.at[n, at * NZ + o], d).wait_recv()
            b = block(zsrc(o), far_y)
            copy(b, b, send_sem, d2d.at[n, 1], d_core).start()

        own = block(z, y)
        copy(x_ref, own, send_sem, zr_s.at[n, 0], d_zr).start()
        copy(x_ref, own, send_sem, zl_s.at[n, 0], d_zl).start()
        emit(0)
        own[...] = x_ref[...]
        before, older = [0], []
        for t in range(8):
            now = [t + 1]
            b = block(zsrc(t + 1), y)
            copy(b, b, send_sem, zr_s.at[n, t], d_zr).wait_recv()
            if t < 7:
                copy(b, b, send_sem, zr_s.at[n, t + 1], d_zr).start()
                b = block(zsrc(15 - t), y)
                copy(b, b, send_sem, zl_s.at[n, t], d_zl).wait_recv()
                if t < 6:
                    copy(b, b, send_sem, zl_s.at[n, t + 1], d_zl).start()
                now.append(15 - t)
            for o in now:
                emit(o)
            for o in before:
                y_arrive(o)
            for o in older:
                h_arrive(o)
            before, older = now, before
        some = panel.at[pl.ds(0, 16 * ROWS)]
        copy(some, some, send_sem, d2d.at[n, 0], d_core).wait_recv()
        after_z()
        for o in before:
            y_arrive(o)
        for o in older + before:
            h_arrive(o)
        some = panel.at[pl.ds(0, 48 * ROWS)]
        copy(some, some, send_sem, d2d.at[n, 1], d_core).wait_recv()

    def gather_done(n, panel):
        most = panel.at[pl.ds(0, 127 * ROWS)]
        copy(most, most, ag_send.at[n], d2d.at[n, 0], d_core).wait_send()

    def exchange(buf, sems, stage, at, devices, value):
        buf[stage, at] = value
        cps = []
        for i, d in enumerate(devices):
            k = stage * 3 + i
            cp = copy(buf.at[stage, at], buf.at[stage, at], sems[0].at[k], sems[1].at[k], d)
            cp.start()
            cps.append(cp)
        return cps

    def exchanged(buf, stage, cps):
        for cp in cps:
            cp.wait_recv()
        return (buf[stage, 0] + buf[stage, 1]) + (buf[stage, 2] + buf[stage, 3])

    def products(panel):
        def slot(s):
            p_hi, p_lo = split(panel[pl.ds(start_ref[s], KALL, stride=16), :])
            t_hi, t_lo = split(tiles_v[s])
            prods[pl.ds(s, KALL, stride=PAD), :] = (
                dot_nt(p_hi, t_hi) + (dot_nt(p_lo, t_hi) + dot_nt(p_hi, t_lo))
            )

        def slots(i, carry):
            for j in range(7):
                slot(i * 7 + j)
            return carry

        lax.fori_loop(0, 6, slots, 0)
        slot(42)

    def reduce_scatter(n, between, after_x, beside, result):
        onehot = (
            lax.broadcasted_iota(jnp.int32, (OUT, 2 * PAD), 0) == local_ref[...]
        ).astype(F32).astype(BF16)
        pending = []
        for q in range(4):
            for kk in range(10):
                k = q * 10 + kk
                hi, lo = split(prods[pl.ds(k * PAD, PAD), :])
                summed = jnp.dot(
                    onehot, jnp.concatenate([hi, lo], axis=0), preferred_element_type=F32
                )
                y_ref[0, k] = summed[: OUT // 2]
                y_ref[1, k] = summed[OUT // 2 :]
            rows_q = pl.ds(q * 10, 10)
            cp = copy(
                y_ref.at[1 - c, rows_q], part.at[n, rows_q], core_s.at[n, q], core_r.at[n, q], d_core
            )
            cp.start()
            pending.append(cp)
        total = y_ref.at[c]
        for q in range(4):
            pending[q].wait_recv()
            rows_q = pl.ds(q * 10, 10)
            total[rows_q] = total[rows_q] + part[n, rows_q]

        def seg(xx, first):
            return total.at[pl.ds(first, 20), pl.ds(pl.multiple_of(xx * 8, 8), 8)]

        lo_half, hi_half = pl.ds(0, 20), pl.ds(20, 20)
        xs, xv = x_s.at[n], x_r.at[n]
        far_r = copy(seg(xf, 0), far.at[n, 0], xs.at[0], xv.at[0], d_xr)
        far_l = copy(seg(xf, 20), far.at[n, 1], xs.at[1], xv.at[1], d_xl)
        near_rb = copy(seg(xr, 20), near.at[n, 0, hi_half], xs.at[2], xv.at[2], d_xr)
        near_la = copy(seg(xl, 0), near.at[n, 1, lo_half], xs.at[3], xv.at[3], d_xl)
        near_ra = copy(seg(xr, 0), near.at[n, 0, lo_half], xs.at[4], xv.at[4], d_xr)
        near_lb = copy(seg(xl, 20), near.at[n, 1, hi_half], xs.at[5], xv.at[5], d_xl)
        pending += [far_r, far_l, near_rb, near_la, near_ra, near_lb]
        far_r.start()
        far_l.start()
        near_rb.start()
        near_la.start()
        between()
        far_r.wait_recv()
        seg(xr, 0)[...] = seg(xr, 0)[...] + far[n, 0]
        near_ra.start()
        far_l.wait_recv()
        seg(xl, 20)[...] = seg(xl, 20)[...] + far[n, 1]
        near_lb.start()
        near_la.wait_recv()
        near_ra.wait_recv()
        low = seg(x, 0)[...] + near[n, 0, lo_half] + near[n, 1, lo_half]
        tail[pl.ds(0, 160)] = low.reshape(160, 128)
        near_rb.wait_recv()
        near_lb.wait_recv()
        high = seg(x, 20)[...] + near[n, 0, hi_half] + near[n, 1, hi_half]
        tail[pl.ds(160, 160)] = high.reshape(160, 128)
        after_x()

        sends = []
        for d in (1, 2, 3):
            to = rem(zlo + d, NZL)
            cp = copy(
                mixed.at[n, pl.ds(pl.multiple_of(to * ROWS, 8), ROWS)], gathered.at[n, d - 1],
                q_s.at[n, d - 1], q_r.at[n, d - 1], d_q[d - 1],
            )
            cp.start()
            sends.append(cp)
        beside()
        for cp in sends:
            cp.wait_recv()
        total_u[n] = (
            mixed[n, pl.ds(pl.multiple_of(zlo * ROWS, 8), ROWS)]
            + gathered[n, 0] + gathered[n, 1] + gathered[n, 2]
        )
        swaps = []
        for k in range(KLOC):
            mine = pl.ds(pl.multiple_of((c * KLOC + k) * 8, 8), 8)
            theirs = pl.ds(pl.multiple_of(((1 - c) * KLOC + k) * 8, 8), 8)
            here = pl.ds(pl.multiple_of(k * 16 + c * 8, 8), 8)
            cp = copy(
                total_u.at[n, theirs], result.at[here], w_s.at[n, k], w_r.at[n, k], d_core
            )
            cp.start()
            swaps.append(cp)
            result[here] = total_u[n, mine]
        for cp in swaps:
            cp.wait_recv()
        return pending + sends + swaps

    def nothing():
        pass

    def plain_tail():
        mixed[0] = tail[...]

    prods[...] = jnp.zeros_like(prods)
    gather(0, x_ref, panel_a, nothing)
    tile_copy.wait()
    products(panel_a)
    sent = reduce_scatter(0, nothing, plain_tail, nothing, image)
    for cp in sent:
        cp.wait_send()

    first = pl.multiple_of(row * 8 * ROWS, 8)
    state = {}

    def whole(b):
        return panel_b[pl.ds(first + b, KALL, stride=16), :]

    def wide(v):
        return jnp.concatenate([v, jnp.zeros((v.shape[0], 128 - v.shape[1]), F32)], axis=1)

    def gram_start():
        gram = jnp.zeros((KALL, KALL), F32)
        for b in range(16):
            v = whole(b)
            gram = gram + exact_nt(v, v)
        state["x"] = exchange(gsum, (g_s, g_r), 0, x, d_x, wide(gram))

    gather(1, image, panel_b, gram_start)
    state["y"] = exchange(gsum, (g_s, g_r), 1, y, d_y, exchanged(gsum, 0, state["x"]))
    products(panel_b)
    state["h"] = exchange(gsum, (g_s, g_r), 2, zh, d_h, exchanged(gsum, 1, state["y"]))

    def factor():
        state["inverse"] = inverse_factor(exchanged(gsum, 2, state["h"]) * (1.0 / ITEMS))

    def mix_tail():
        for j in range(8):
            at = pl.ds(j, KALL, stride=8)
            mixed[1, at, :] = exact(state["inverse"], tail[at, :])

    def write_basis():
        for b in range(16):
            basis_all[pl.ds(b, KALL, stride=16), :] = exact(state["inverse"], whole(b))
        basis_ref[...] = basis_all[pl.ds(pl.multiple_of(cut * ROWS, 8), ROWS), :]

    sent = reduce_scatter(1, factor, mix_tail, write_basis, product)

    local = jnp.zeros((KLOC, KALL), F32)
    for b in range(16):
        local = local + exact_nt(
            product[pl.ds(b, KLOC, stride=16), :], basis_all[pl.ds(b, KALL, stride=16), :]
        )
    local = jnp.concatenate([wide(local), jnp.zeros((3, 128), F32)], axis=0)
    p_sems = (p_s, p_r)
    px = exchange(psum, p_sems, 0, x, d_x, local)
    py = exchange(psum, p_sems, 1, y, d_y, exchanged(psum, 0, px))
    ph = exchange(psum, p_sems, 2, zh, d_h, exchanged(psum, 1, py))
    projected = exchanged(psum, 2, ph)[:KLOC, :KALL] * (1.0 / ITEMS)
    for b in range(16):
        at = pl.ds(b, KLOC, stride=16)
        residual_ref[at, :] = product[at, :] - exact(
            projected, basis_all[pl.ds(b, KALL, stride=16), :]
        )

    for cp in sent + state["x"] + state["y"] + state["h"] + px + py + ph:
        cp.wait_send()
    gather_done(0, panel_a)
    gather_done(1, panel_b)


def shards(warm, tiles, tile_rows, tile_cols):
    local = tile_rows - lax.axis_index("row") * OUT
    local = jnp.where(
        local >= 0, local % 16 // 8 * 32 + local // 16 * 8 + local % 8, -1
    )
    local = jnp.pad(local, (0, PAD - SLOTS), constant_values=-1)
    local = jnp.concatenate([local, local]).reshape(1, 2 * PAD)
    start = tile_cols // 64 * (8 * ROWS) + tile_cols % 16
    dma = pltpu.SemaphoreType.DMA
    vmem = pl.BlockSpec(memory_space=pltpu.VMEM)
    basis, residual = pl.pallas_call(
        kernel,
        name="operator_steps",
        out_shape=(jax.ShapeDtypeStruct((ROWS, 128), F32),) * 2,
        in_specs=[
            vmem,
            pl.BlockSpec(memory_space=pl.ANY),
            pl.BlockSpec(memory_space=pltpu.SMEM),
            vmem,
        ],
        out_specs=(vmem, vmem),
        scratch_shapes=[
            pltpu.VMEM((SLOTS, 128, 128), F32),
            pltpu.VMEM((128 * ROWS, 128), F32),
            pltpu.VMEM((128 * ROWS, 128), F32),
            pltpu.VMEM((KALL * PAD, 128), F32),
            pltpu.VMEM((2, KALL, OUT // 2, 128), F32),
            pltpu.VMEM((2, KALL, OUT // 2, 128), F32),
            pltpu.VMEM((2, 2, 20, 8, 128), F32),
            pltpu.VMEM((2, 2, KALL, 8, 128), F32),
            pltpu.VMEM((KALL * 8, 128), F32),
            pltpu.VMEM((2, KALL * 8, 128), F32),
            pltpu.VMEM((2, 3, ROWS, 128), F32),
            pltpu.VMEM((2, ROWS, 128), F32),
            pltpu.VMEM((ROWS, 128), F32),
            pltpu.VMEM((ROWS, 128), F32),
            pltpu.VMEM((KALL * 16, 128), F32),
            pltpu.VMEM((3, 4, KALL, 128), F32),
            pltpu.VMEM((3, 4, 8, 128), F32),
            dma, dma((2,)), dma((2, 8)), dma((2, 7)), dma((2, 32)), dma((2, 32)), dma((2, 2)),
            dma((2, 4)), dma((2, 4)), dma((2, 6)), dma((2, 6)), dma((2, 3)), dma((2, 3)),
            dma((2, 5)), dma((2, 5)), dma((9,)), dma((9,)), dma((9,)), dma((9,)),
        ],
        compiler_params=pltpu.CompilerParams(collective_id=0, has_side_effects=True),
    )(warm.reshape(ROWS, 128), tiles, start, local)
    return basis.reshape(KLOC, 2048), residual.reshape(KLOC, 2048)


def solution(mesh):
    return jax.shard_map(
        shards,
        mesh=mesh,
        in_specs=(
            P("cuts", ("row", "col")),
            P(("row", "col", "cuts"), None, None),
            P(("row", "col", "cuts")),
            P(("row", "col", "cuts")),
        ),
        out_specs=(P("cuts", ("row", "col")), P("cuts", ("row", "col"))),
        check_vma=False,
    )
```
